32 devices in a mesh: parts: 2 (over y), modes: 16 (over z, x, core).
Axes of the slice: x: 2, y: 2, z: 4, core: 2. Of those that a mesh axis runs over, the one named last changes fastest.
Arguments:
- stem: bfloat16 [2, 16, 64, 32, 512], P(None, 'modes', None, None, 'parts'), parts along dimension 4, may hold values from -6 to 6
- branch_one: bfloat16 [2, 1024, 1024], replicated, may hold values from -0.125 to 0.125
- branch_two: bfloat16 [2, 1024, 1024], replicated, may hold values from -0.125 to 0.125
- branch_three: bfloat16 [2, 2, 16, 512, 512], P(None, None, 'modes'), may hold values from -0.0625 to 0.0625
- leg_orders: int32 [2, 10], replicated, may hold values from 0 to 9, each once within a row
- slice_pick: int32 [32], P('parts'), parts along dimension 0, may hold values from 0 to 1
Outputs:
- contracted: bfloat16 [1024, 2, 2, 2, 256], P(('parts', 'modes')), parts along dimension 0
The draws below stay inside these ranges and needn't reach their ends.
There are 2 independent parts, one for each index of `parts`. The reference program is written for one: setup_inputs(seed, part) draws one part's arguments, and reference() takes and returns one part's arrays. A program takes and returns all parts, laid end to end along the dimension named above; an argument that names none is the same for every part. Nothing has to cross between parts.
Inputs may be any that keep to these rules, and one draw needn't show every extreme that they name: `leg_orders`: each row names every input leg bit once.
All inputs are finite; a program needn't handle non-finite values.
Results may differ from the reference program's by a relative error of at most 0.008.
Values may be sent and summed in bfloat16 or wider, within the bound.
No kernel may reach another device: no remote copies, remote signals or barrier semaphores. Data moves between devices by JAX's collectives and lax.ppermute only.
A program may use at most 128 MiB of HBM per device.

```python
import jax
import jax.numpy as jnp

LEGS = 10
C = 1024
OUTW = 512
SLICES = 2
ROWS_DEV = 2
L = 256
E = 64
H = 32
N_MODES = 16


def with_ends(values, own_key, low, top_value):
    shape = values.shape
    place = [jax.random.randint(jax.random.fold_in(own_key, axis), (), 0, shape[axis]) for axis in range(len(shape))]
    values = values.at[tuple(place)].set(low)
    longest = shape.index(max(shape))
    place[longest] = (place[longest] + 1) % shape[longest]
    return values.at[tuple(place)].set(top_value)


def raised(drawn, key, source, target, blocks, factor):
    def block_of(dim):
        return (jnp.arange(drawn.shape[dim]) // (drawn.shape[dim] // blocks)).reshape((-1,) + (1,) * (drawn.ndim - 1 - dim))

    one_side = jax.random.permutation(key, blocks)[block_of(target)]
    other_side = (block_of(target) + blocks // 2) % blocks
    return jnp.where((block_of(source) == one_side) | (block_of(source) == other_side), factor * drawn, drawn)


def levels(stream_key, extent, shards, low, largest):
    def one(axis_at, parts):
        heights = jax.random.uniform(jax.random.fold_in(jax.random.fold_in(stream_key, 6), axis_at), (parts,), jnp.float32, low / len(shards), largest / len(shards))
        return jnp.repeat(jnp.exp(heights), extent[axis_at] // parts).reshape((-1,) + (1,) * (len(extent) - axis_at - 1))

    factor_of = one(*shards[0])
    for cut in shards[1:]:
        factor_of = factor_of * one(*cut)
    return factor_of


def bell_draw(rng, shape, deviation, bound, shards=(), kind=jnp.bfloat16):
    gain = levels(rng, shape, shards, -0.22, 0.18) if shards else 1.0
    drawn = jax.random.normal(rng, shape, jnp.float32) * deviation * gain
    return jnp.minimum(jnp.maximum(drawn, -bound), bound).astype(kind)


def gaussian_with(key, dims, width, most, pieces, heavy, kind=jnp.bfloat16):
    values = width * jax.random.normal(key, dims, jnp.float32)
    if pieces:
        values = values * levels(key, dims, pieces, -0.22, 0.18)
    return jnp.clip(raised(values, jax.random.fold_in(key, 3), *heavy), -most, most).astype(kind)


def setup_inputs(seed: int = 0, part: int = 0) -> dict:
    splits = jax.random.split(jax.random.key(seed), 7)
    own_keys = jax.random.split(jax.random.fold_in(splits[6], part), 7)
    stem = bell_draw(own_keys[0], (2, N_MODES, E, H, L), 1.0, 6.0, ((1, 16),))
    branch_one = bell_draw(splits[1], (2, C, C), (2 * C) ** -0.5, 0.125)
    branch_two = bell_draw(splits[2], (2, C, C), (2 * C) ** -0.5, 0.125)
    branch_three = gaussian_with(splits[3], (SLICES, 2, N_MODES, OUTW, C // 2), (N_MODES * C) ** -0.5, 0.0625, ((2, 16),), (2, 3, 16, 2.0))
    leg_orders = jax.vmap(lambda own: jax.random.permutation(own, LEGS))(jax.random.split(splits[4], 2)).reshape((2, LEGS)).astype(jnp.int32)
    slice_pick = with_ends(jax.random.randint(own_keys[5], (N_MODES,), 0, SLICES), jax.random.fold_in(own_keys[5], 1), 0, SLICES - 1).astype(jnp.int32)
    return dict(stem=stem, branch_one=branch_one, branch_two=branch_two, branch_three=branch_three, leg_orders=leg_orders, slice_pick=slice_pick)


def leg_index(order, leg_width):
    positions = jnp.arange(leg_width, dtype=jnp.int32)
    shifts = jnp.arange(order.shape[0], dtype=jnp.int32)
    digits = jnp.right_shift(positions[:, None], shifts[None, :]) % 2
    placed = jnp.left_shift(digits, order[None, :].astype(jnp.int32))
    return jnp.sum(placed, axis=1).astype(jnp.int32)


def complex_apply(weight, values):
    real_part = weight[0]
    imag_part = weight[1]
    block_matrix = jnp.concatenate([jnp.concatenate([real_part, -imag_part], axis=1), jnp.concatenate([imag_part, real_part], axis=1)], axis=0)
    stacked = values.reshape(2 * values.shape[1], values.shape[2])
    result = jnp.dot(block_matrix, stacked, preferred_element_type=jnp.float32)
    return result.reshape(2, weight.shape[1], values.shape[2])


def reference(stem, branch_one, branch_two, branch_three, leg_orders, slice_pick):
    groups = N_MODES
    half_width = C // 2
    quarter = groups // 4
    columns = ROWS_DEV * groups * L
    values = stem.reshape(2, C, columns)
    weight_one = jnp.take(branch_one, leg_index(leg_orders[0], C), axis=2)
    after_first = complex_apply(weight_one, values).astype(jnp.bfloat16)
    after_first = after_first.reshape(2, 2, half_width, 2, quarter, 2, ROWS_DEV, L)
    second_in = after_first.transpose(0, 3, 2, 1, 4, 5, 6, 7).reshape(2, C, columns)
    weight_two = jnp.take(branch_two, leg_index(leg_orders[1], C), axis=2)
    after_second = complex_apply(weight_two, second_in).astype(jnp.bfloat16)
    after_second = after_second.reshape(2, 2, half_width, 2, quarter, 2, ROWS_DEV, L)
    third_in = after_second.transpose(0, 3, 4, 6, 2, 1, 5, 7).reshape(2, groups * half_width, 4 * L)
    split_ids = jnp.arange(groups, dtype=jnp.int32)
    picked = branch_three[slice_pick.astype(jnp.int32), :, split_ids]
    chosen = picked.transpose(1, 0, 2, 3)
    weight_three = chosen.transpose(0, 2, 1, 3).reshape(2, OUTW, groups * half_width)
    after_third = complex_apply(weight_three, third_in)
    return after_third.reshape(2, OUTW, 2, 2, L).transpose(1, 0, 2, 3, 4).astype(jnp.bfloat16)
```

```python
import jax
import jax.numpy as jnp
from jax import lax
from jax.experimental import pallas as pl
from jax.experimental.pallas import tpu as pltpu
from jax.sharding import PartitionSpec as P

BF = jnp.bfloat16
F32 = jnp.float32


def dot(lhs, rhs):
    return jnp.dot(lhs, rhs, preferred_element_type=F32)


def one_hot(orders_ref, row, start, width, leg_width):
    legs = leg_width.bit_length() - 1
    index = lax.broadcasted_iota(jnp.int32, (1, width), 1) + start
    placed = jnp.zeros((1, width), jnp.int32)
    for bit in range(legs):
        placed += jnp.left_shift(jnp.right_shift(index, bit) & 1, orders_ref[row, bit])
    rows = lax.broadcasted_iota(jnp.int32, (leg_width, width), 0)
    return jnp.where(rows == placed, 1.0, 0.0).astype(BF)


def turn_kernel(half_ref, orders_ref, one_ref, two_ref, out_one_ref, out_two_ref, pick_one, pick_two):
    leg_width = one_ref.shape[2]
    width = leg_width // 2

    @pl.when((pl.program_id(0) == 0) & (pl.program_id(1) == 0))
    def _():
        pick_one[...] = one_hot(orders_ref, 0, half_ref[0] * width, width, leg_width)
        pick_two[...] = one_hot(orders_ref, 1, 0, leg_width, leg_width)

    out_one_ref[0] = dot(one_ref[0], pick_one[...]).astype(BF)
    out_two_ref[0] = dot(two_ref[0], pick_two[...]).astype(BF)


def turned(half, orders, one, two):
    leg_width = one.shape[2]
    width = leg_width // 2
    rows = 256
    spec = lambda wide: pl.BlockSpec((1, rows, wide), lambda r, i, *_: (r, i, 0))
    return pl.pallas_call(
        turn_kernel,
        grid_spec=pltpu.PrefetchScalarGridSpec(
            num_scalar_prefetch=2,
            grid=(2, leg_width // rows),
            in_specs=[spec(leg_width), spec(leg_width)],
            out_specs=[spec(width), spec(leg_width)],
            scratch_shapes=[pltpu.VMEM((leg_width, width), BF), pltpu.VMEM((leg_width, leg_width), BF)],
        ),
        out_shape=[
            jax.ShapeDtypeStruct((2, leg_width, width), BF),
            jax.ShapeDtypeStruct((2, leg_width, leg_width), BF),
        ],
        name="turn",
    )(half, orders, one, two)


def complex_dot(wr, wi, vr, vi):
    return dot(wr, vr) - dot(wi, vi), dot(wr, vi) + dot(wi, vr)


def chain_kernel(x_ref, one_ref, two_ref, out_ref, first):
    half = one_ref.shape[1] // 2
    lanes = x_ref.shape[5]
    inner = x_ref.shape[0] * x_ref.shape[4]

    def step_one(n, _):
        a, d, t = n >> 2, (n >> 1) & 1, n & 1
        rows = pl.ds(pl.multiple_of(t * half, half), half)
        vr = x_ref[:, 0, a, d].reshape(inner, lanes)
        vi = x_ref[:, 1, a, d].reshape(inner, lanes)
        yr, yi = complex_dot(one_ref[0, rows, :], one_ref[1, rows, :], vr, vi)
        first[a, t, d, 0] = yr.astype(BF)
        first[a, t, d, 1] = yi.astype(BF)
        return 0

    lax.fori_loop(0, 8, step_one, 0)

    def step_two(n, _):
        t, d, u = n >> 2, (n >> 1) & 1, n & 1
        rows = pl.ds(pl.multiple_of(u * half, half), half)
        vr = first[:, t, d, 0].reshape(2 * half, lanes)
        vi = first[:, t, d, 1].reshape(2 * half, lanes)
        yr, yi = complex_dot(two_ref[0, rows, :], two_ref[1, rows, :], vr, vi)
        out_ref[t, d, 0, u] = yr.astype(BF)
        out_ref[t, d, 1, u] = yi.astype(BF)
        return 0

    lax.fori_loop(0, 8, step_two, 0)


def chained(x, one, two):
    half = one.shape[1] // 2
    lanes = x.shape[5]
    return pl.pallas_call(
        chain_kernel,
        out_shape=jax.ShapeDtypeStruct((2, 2, 2, 2, half, lanes), BF),
        scratch_shapes=[pltpu.VMEM((2, 2, 2, 2, half, lanes), BF)],
        name="chain",
    )(x, one, two)


def join_kernel(place_ref, w0, w1, w2, w3, v_ref, out_ref):
    lanes = v_ref.shape[5]
    t0, d0 = place_ref[0], place_ref[1]
    spots = ((t0, d0), (1 - t0, d0), (t0, 1 - d0), (1 - t0, 1 - d0))
    weights = (w0, w1, w2, w3)
    wr = jnp.concatenate([w[0] for w in weights], axis=1)
    wi = jnp.concatenate([w[1] for w in weights], axis=1)
    for u in range(2):
        vr = jnp.concatenate([v_ref[t, d, 0, u] for t, d in spots], axis=0)
        vi = jnp.concatenate([v_ref[t, d, 1, u] for t, d in spots], axis=0)
        yr, yi = complex_dot(wr, wi, vr, vi)
        out_ref[:, u * lanes:(u + 1) * lanes] = yr.astype(BF)
        out_ref[:, (2 + u) * lanes:(3 + u) * lanes] = yi.astype(BF)


def joined(place, weights, v):
    smem = pl.BlockSpec(memory_space=pltpu.SMEM)
    vmem = pl.BlockSpec(memory_space=pltpu.VMEM)
    return pl.pallas_call(
        join_kernel,
        in_specs=[smem] + [vmem] * 5,
        out_shape=jax.ShapeDtypeStruct((weights[0].shape[1], 4 * v.shape[5]), BF),
        name="join",
    )(place, *weights, v)


def per_device(stem, branch_one, branch_two, branch_three, leg_orders, slice_pick):
    groups = lax.axis_size("modes")
    own = lax.axis_index("modes")
    side = groups // 2
    extent = stem.shape[2]
    lanes = stem.shape[4]
    top = own // side
    core = own % 2

    pieces = stem.reshape(2, extent, 2, side, 2, lanes).transpose(3, 0, 2, 4, 1, 5)
    halves = [list(range(side)), list(range(side, groups))]
    arrived = lax.all_to_all(pieces, "modes", 0, 0, tiled=True, axis_index_groups=halves)
    if extent % 16:
        arrived = arrived.transpose(1, 2, 3, 0, 4, 5).reshape(1, 2, 2, 2, side * extent, lanes)

    own_pick = lax.dynamic_index_in_dim(slice_pick, own, 0, keepdims=False)
    chosen = lax.dynamic_index_in_dim(branch_three, own_pick, 0, keepdims=False)[:, 0]
    across = [(i, i ^ side) for i in range(groups)]
    beside = [(i, i ^ 1) for i in range(groups)]
    other = lax.ppermute(chosen, "modes", across)
    chosen_beside = lax.ppermute(chosen, "modes", beside)
    other_beside = lax.ppermute(other, "modes", beside)

    one, two = turned(top.reshape(1).astype(jnp.int32), leg_orders, branch_one, branch_two)
    v = chained(arrived, one, two)
    place = jnp.stack([top, core]).astype(jnp.int32)
    partial = joined(place, (chosen, other, chosen_beside, other_beside), v)

    out_width = partial.shape[0]
    share = out_width // groups
    spread = lax.all_to_all(partial.reshape(groups, share, 4 * lanes), "modes", 0, 0, tiled=True)
    spread = spread.reshape(side, 2, share, 2, 2, lanes).astype(F32)
    return jnp.sum(spread, axis=0).astype(BF).transpose(1, 2, 3, 0, 4)


def solution(mesh):
    in_specs = (
        P(None, "modes", None, None, "parts"),
        P(),
        P(),
        P(None, None, "modes", None, None),
        P(),
        P("parts"),
    )
    out_specs = P(("parts", "modes"), None, None, None, None)
    return jax.shard_map(
        per_device, mesh=mesh, in_specs=in_specs, out_specs=out_specs, check_vma=False
    )
```

```python
import jax
import jax.numpy as jnp
from jax import lax
from jax.experimental import pallas as pl
from jax.experimental.pallas import tpu as pltpu
from jax.sharding import PartitionSpec as P


BF = jnp.bfloat16
F32 = jnp.float32


def dot(lhs, rhs):
    return jnp.dot(lhs, rhs, preferred_element_type=F32)


def copies(sem, *pairs):
    return [pltpu.make_async_copy(src, dst, sem.at[n]) for n, (src, dst) in enumerate(pairs)]


def anywhere(count):
    return [pl.BlockSpec(memory_space=pl.ANY) for _ in range(count)]


def complex_dot(wr, wi, vr, vi):
    return dot(wr, vr) - dot(wi, vi), dot(wr, vi) + dot(wi, vr)


def turn_kernel(row, start_ref, orders_ref, branch_hbm, out_hbm, branch, out, pick, sem, out_sem):
    leg_width, width = pick.shape
    half = leg_width // 2
    pieces = [(r, pl.ds(u * half, half)) for r in range(2) for u in range(2)]
    loads = copies(sem, *[(branch_hbm.at[r, rows], branch.at[r, rows]) for r, rows in pieces])
    stores = copies(out_sem, *[(out.at[r, rows], out_hbm.at[r, rows]) for r, rows in pieces])
    for load in loads:
        load.start()

    index = lax.broadcasted_iota(jnp.int32, (1, width), 1) + start_ref[0]
    placed = jnp.zeros((1, width), jnp.int32)
    for bit in range(leg_width.bit_length() - 1):
        placed += jnp.left_shift(jnp.right_shift(index, bit) & 1, orders_ref[row, bit])
    ahead = placed - lax.broadcasted_iota(jnp.int32, (16, width), 0)

    def build(n, _):
        base = pl.multiple_of(n * 16, 16)
        pick[pl.ds(base, 16), :] = jnp.where(ahead == base, 1.0, 0.0).astype(BF)
        return 0

    lax.fori_loop(0, leg_width // 16, build, 0)
    for (r, rows), load, store in zip(pieces, loads, stores):
        load.wait()
        out[r, rows, :] = dot(branch[r, rows, :], pick[...]).astype(BF)
        store.start()
    for store in stores:
        store.wait()


def turned(row, start, width, orders, branch):
    leg_width = branch.shape[2]
    smem = pl.BlockSpec(memory_space=pltpu.SMEM)
    return pl.pallas_call(
        lambda *refs: turn_kernel(row, *refs),
        in_specs=[smem, smem] + anywhere(1),
        out_specs=anywhere(1)[0],
        out_shape=jax.ShapeDtypeStruct((2, leg_width, width), BF),
        scratch_shapes=[
            pltpu.VMEM(branch.shape, BF),
            pltpu.VMEM((2, leg_width, width), BF),
            pltpu.VMEM((leg_width, width), BF),
            pltpu.SemaphoreType.DMA((4,)),
            pltpu.SemaphoreType.DMA((4,)),
        ],
        cost_estimate=pl.CostEstimate(flops=4 * width * leg_width**2, transcendentals=0, bytes_accessed=4 * leg_width**2),
        name="turn",
    )(start, orders, branch)


def chain_kernel(place_ref, x_hbm, one_hbm, two_hbm, *refs):
    held_hbm, (v_hbm, part_hbm) = refs[:2], refs[2:4]
    x, one, two, held, first, v, part, x_sem, one_sem, two_sem, held_sem, v_sem, part_sem = refs[4:]
    half = one.shape[1] // 2
    lanes = x.shape[5]
    inner = x.shape[2] * x.shape[4]
    halves = [pl.ds(u * half, half) for u in range(2)]
    t0, d0 = place_ref[0], place_ref[1]
    spots = [(d, a) for d in range(2) for a in range(2)]
    x_loads = copies(x_sem, *[(x_hbm.at[:, :, a, d], x.at[d, a]) for d, a in spots])
    one_loads = copies(one_sem, *[(one_hbm.at[:, rows], one.at[:, rows]) for rows in halves])
    two_loads = copies(two_sem, *[(two_hbm.at[:, rows], two.at[:, rows]) for rows in halves])
    held_loads = copies(held_sem, *[(held_hbm[n], held.at[:, :, pl.ds(n * half, half)]) for n in range(2)])
    x_loads[0].start()
    one_loads[0].start()
    for load in x_loads[1:] + one_loads[1:] + two_loads + held_loads:
        load.start()

    for t in range(2):
        one_loads[t].wait()
        for d, a in spots:
            if t == 0:
                x_loads[2 * d + a].wait()
            vr = x[d, a, :, 0].reshape(inner, lanes)
            vi = x[d, a, :, 1].reshape(inner, lanes)
            yr, yi = complex_dot(one[0, halves[t], :], one[1, halves[t], :], vr, vi)
            first[d, a, t, 0] = yr.astype(BF)
            first[d, a, t, 1] = yi.astype(BF)

    v_stores = copies(v_sem, *[(v.at[1 - t0, :, :, u], v_hbm.at[:, :, u]) for u in range(2)])
    for u in range(2):
        two_loads[u].wait()

        def step_two(n, _):
            t, d = jnp.where(n < 2, 1 - t0, t0), n & 1
            vr = first[d, :, t, 0].reshape(2 * half, lanes)
            vi = first[d, :, t, 1].reshape(2 * half, lanes)
            yr, yi = complex_dot(two[0, halves[u], :], two[1, halves[u], :], vr, vi)
            v[t, d, 0, u] = yr.astype(BF)
            v[t, d, 1, u] = yi.astype(BF)
            return 0

        lax.fori_loop(0, 4, step_two, 0)
        v_stores[u].start()

    for load in held_loads:
        load.wait()
    part_stores = copies(part_sem, *[(part.at[u], part_hbm.at[u]) for u in range(2)])
    for u in range(2):
        vr = jnp.concatenate([v[t0, d0, 0, u], v[t0, 1 - d0, 0, u]], axis=0)
        vi = jnp.concatenate([v[t0, d0, 1, u], v[t0, 1 - d0, 1, u]], axis=0)
        part[u, 0], part[u, 1] = complex_dot(held[0], held[1], vr, vi)
        part_stores[u].start()
    for store in v_stores + part_stores:
        store.wait()


def chained(place, x, one, two, held):
    half = one.shape[1] // 2
    lanes = x.shape[5]
    rows = held[0].shape[1]
    v_shape = (2, 2, 2, half, lanes)
    part_shape = (2, 2, rows, lanes)
    sems = lambda count: pltpu.SemaphoreType.DMA((count,))
    return pl.pallas_call(
        chain_kernel,
        in_specs=[pl.BlockSpec(memory_space=pltpu.SMEM)] + anywhere(5),
        out_specs=anywhere(2),
        out_shape=[jax.ShapeDtypeStruct(v_shape, BF), jax.ShapeDtypeStruct(part_shape, F32)],
        scratch_shapes=[
            pltpu.VMEM((2, 2) + x.shape[:2] + x.shape[4:], BF),
            pltpu.VMEM(one.shape, BF),
            pltpu.VMEM(two.shape, BF),
            pltpu.VMEM((2, rows, 2 * half), BF),
            pltpu.VMEM((2,) + v_shape, BF),
            pltpu.VMEM((2,) + v_shape, BF),
            pltpu.VMEM(part_shape, F32),
        ] + [sems(4), sems(2), sems(2), sems(2), sems(2), sems(2)],
        cost_estimate=pl.CostEstimate(flops=112 * half * half * 2 * lanes, transcendentals=0, bytes_accessed=72 * half**2),
        name="chain",
    )(place, x, one, two, *held)


def join_kernel(place_ref, *refs):
    weights_hbm, (v_hbm, part_hbm, out), (w, v, part, sem) = refs[:2], refs[2:5], refs[5:]
    lanes = v.shape[4]
    inner = w.shape[2] // 2
    d0 = place_ref[1]
    w_loads = copies(sem, *[(weights_hbm[n], w.at[:, :, pl.ds(n * inner, inner)]) for n in range(2)])
    v_loads = [pltpu.make_async_copy(v_hbm.at[:, :, u], v.at[:, :, u], sem.at[2 + u]) for u in range(2)]
    p_loads = [pltpu.make_async_copy(part_hbm.at[u], part.at[u], sem.at[4 + u]) for u in range(2)]
    for load in [v_loads[0]] + w_loads + [p_loads[0], v_loads[1], p_loads[1]]:
        load.start()
    for load in w_loads:
        load.wait()
    for u in range(2):
        v_loads[u].wait()
        vr = jnp.concatenate([v[d0, 0, u], v[1 - d0, 0, u]], axis=0)
        vi = jnp.concatenate([v[d0, 1, u], v[1 - d0, 1, u]], axis=0)
        p_loads[u].wait()
        yr, yi = complex_dot(w[0], w[1], vr, vi)
        for r, y in enumerate((yr, yi)):
            out[:, (2 * r + u) * lanes:(2 * r + u + 1) * lanes] = (part[u, r] + y).astype(BF)


def joined(place, weights, v, part):
    rows, inner = weights[0].shape[1:]
    lanes = v.shape[4]
    return pl.pallas_call(
        join_kernel,
        in_specs=[pl.BlockSpec(memory_space=pltpu.SMEM)] + anywhere(4),
        out_specs=pl.BlockSpec(memory_space=pltpu.VMEM),
        out_shape=jax.ShapeDtypeStruct((rows, 4 * lanes), BF),
        scratch_shapes=[
            pltpu.VMEM((2, rows, 2 * inner), BF),
            pltpu.VMEM(v.shape, BF),
            pltpu.VMEM(part.shape, F32),
            pltpu.SemaphoreType.DMA((6,)),
        ],
        cost_estimate=pl.CostEstimate(flops=32 * rows * inner * lanes, transcendentals=0, bytes_accessed=24 * rows * inner),
        name="join",
    )(place, *weights, v, part)


def pick_kernel(own_ref, pick_ref, branch_hbm, out_hbm, held, sem, out_sem):
    spot = pick_ref[own_ref[0]]
    loads = copies(sem, *[(branch_hbm.at[spot, r, 0], held.at[r]) for r in range(2)])
    stores = copies(out_sem, *[(held.at[r], out_hbm.at[r]) for r in range(2)])
    for load in loads:
        load.start()
    for load, store in zip(loads, stores):
        load.wait()
        store.start()
    for store in stores:
        store.wait()


def picked(own, slice_pick, branch):
    smem = pl.BlockSpec(memory_space=pltpu.SMEM)
    return pl.pallas_call(
        pick_kernel,
        in_specs=[smem, smem] + anywhere(1),
        out_specs=anywhere(1)[0],
        out_shape=jax.ShapeDtypeStruct(branch.shape[1:2] + branch.shape[3:], BF),
        scratch_shapes=[
            pltpu.VMEM(branch.shape[1:2] + branch.shape[3:], BF),
            pltpu.SemaphoreType.DMA((2,)),
            pltpu.SemaphoreType.DMA((2,)),
        ],
        cost_estimate=pl.CostEstimate(flops=0, transcendentals=0, bytes_accessed=2 * branch.size),
        name="pick",
    )(own.reshape(1).astype(jnp.int32), slice_pick, branch)


def per_device(stem, branch_one, branch_two, branch_three, leg_orders, slice_pick):
    groups = lax.axis_size("modes")
    own = lax.axis_index("modes")
    side = groups // 2
    quarter = groups // 4
    extent = stem.shape[2]
    lanes = stem.shape[4]
    leg_width = branch_one.shape[2]
    top = own // side
    core = own % 2
    middle = (own // quarter == 1) | (own // quarter == 2)

    beside = [(i, i ^ 1) for i in range(groups)]
    swap = [(a * quarter + i, b * quarter + i) for a, b in ((1, 2), (2, 1)) for i in range(quarter)]
    cycle = [(a * quarter + i, b * quarter + i) for a, b in ((0, 2), (2, 3), (3, 1), (1, 0)) for i in range(quarter)]

    chosen = picked(own, slice_pick, branch_three)
    out_width = chosen.shape[1]
    share = out_width // groups
    chosen, stem = lax.optimization_barrier((chosen, stem))

    def move(value, route):
        return lax.ppermute(value, "modes", route)

    swapped = move(chosen, swap)
    near = move(chosen, beside)

    pieces = stem.reshape(2, extent, 2, side, 2, lanes).transpose(3, 0, 2, 4, 1, 5)
    halves = [list(range(side)), list(range(side, groups))]
    arrived = lax.all_to_all(pieces, "modes", 0, 0, tiled=True, axis_index_groups=halves)
    if extent % 16:
        arrived = arrived.transpose(1, 2, 3, 0, 4, 5).reshape(1, 2, 2, 2, side * extent, lanes)

    start = (top * (leg_width // 2)).reshape(1).astype(jnp.int32)
    place = jnp.stack([top, core]).astype(jnp.int32)
    one = turned(0, start, leg_width // 2, leg_orders, branch_one)
    two = turned(1, jnp.zeros_like(start), leg_width, leg_orders, branch_two)
    swapped, one, two = lax.optimization_barrier((swapped, one, two))
    other = move(jnp.where(middle, swapped, chosen), cycle)
    v, part = chained(place, arrived, one, two, (chosen, near))
    other, v = lax.optimization_barrier((other, v))
    far = move(other, beside)
    partial = joined(place, (other, far), v, part)
    spread = lax.all_to_all(partial.reshape(groups, share, 4 * lanes), "modes", 0, 0, tiled=True)
    total = jnp.sum(spread.reshape(side, 2, share, 4 * lanes).astype(F32), axis=0).astype(BF)
    return total.reshape(2, share, 2, 2, lanes).transpose(1, 2, 3, 0, 4)


def solution(mesh):
    in_specs = (
        P(None, "modes", None, None, "parts"),
        P(),
        P(),
        P(None, None, "modes", None, None),
        P(),
        P("parts"),
    )
    out_specs = P(("parts", "modes"), None, None, None, None)

    return jax.shard_map(per_device, mesh=mesh, in_specs=in_specs, out_specs=out_specs, check_vma=False)
```

```python
import jax
import jax.numpy as jnp
from jax import lax
from jax.experimental import pallas as pl
from jax.experimental.pallas import tpu as pltpu
from jax.sharding import PartitionSpec as P


BF = jnp.bfloat16
F32 = jnp.float32


def dot(lhs, rhs):
    return jnp.dot(lhs, rhs, preferred_element_type=F32)


def copies(sem, *pairs):
    return [pltpu.make_async_copy(src, dst, sem.at[n]) for n, (src, dst) in enumerate(pairs)]


def params(mib):
    return pltpu.CompilerParams(vmem_limit_bytes=mib << 20)


def inside(count):
    return [pl.BlockSpec(memory_space=pltpu.VMEM) for _ in range(count)]


def anywhere(count):
    return [pl.BlockSpec(memory_space=pl.ANY) for _ in range(count)]


def complex_dot(wr, wi, vr, vi):
    return dot(wr, vr) - dot(wi, vi), dot(wr, vi) + dot(wi, vr)


def turn_kernel(row, start_ref, orders_ref, branch_hbm, out_hbm, branch, out, pick, sem, out_sem):
    leg_width, width = pick.shape
    half = leg_width // 2
    pieces = [(r, pl.ds(u * half, half)) for r in range(2) for u in range(2)]
    loads = copies(sem, *[(branch_hbm.at[r, rows], branch.at[r, rows]) for r, rows in pieces])
    stores = copies(out_sem, *[(out.at[r, rows], out_hbm.at[r, rows]) for r, rows in pieces])
    for load in loads:
        load.start()

    index = lax.broadcasted_iota(jnp.int32, (1, width), 1) + start_ref[0]
    placed = jnp.zeros((1, width), jnp.int32)
    for bit in range(leg_width.bit_length() - 1):
        placed += jnp.left_shift(jnp.right_shift(index, bit) & 1, orders_ref[row, bit])
    ahead = placed - lax.broadcasted_iota(jnp.int32, (16, width), 0)

    def build(n, _):
        base = pl.multiple_of(n * 16, 16)
        pick[pl.ds(base, 16), :] = jnp.where(ahead == base, 1.0, 0.0).astype(BF)
        return 0

    lax.fori_loop(0, leg_width // 16, build, 0)
    for (r, rows), load, store in zip(pieces, loads, stores):
        load.wait()
        out[r, rows, :] = dot(branch[r, rows, :], pick[...]).astype(BF)
        store.start()
    for store in stores:
        store.wait()


def turned(row, start, width, orders, branch):
    leg_width = branch.shape[2]
    smem = pl.BlockSpec(memory_space=pltpu.SMEM)
    return pl.pallas_call(
        lambda *refs: turn_kernel(row, *refs),
        in_specs=[smem, smem] + anywhere(1),
        out_specs=anywhere(1)[0],
        out_shape=jax.ShapeDtypeStruct((2, leg_width, width), BF),
        scratch_shapes=[
            pltpu.VMEM(branch.shape, BF),
            pltpu.VMEM((2, leg_width, width), BF),
            pltpu.VMEM((leg_width, width), BF),
            pltpu.SemaphoreType.DMA((4,)),
            pltpu.SemaphoreType.DMA((4,)),
        ],
        cost_estimate=pl.CostEstimate(flops=4 * width * leg_width**2, transcendentals=0, bytes_accessed=4 * leg_width**2),
        compiler_params=params(16),
        name="turn",
    )(start, orders, branch)


def chain_kernel(place_ref, x, one_hbm, two_hbm, *refs):
    held_hbm, (v_out, part) = refs[:2], refs[2:4]
    one, two, held, first, v, one_sem, two_sem, held_sem = refs[4:]
    half = one.shape[1] // 2
    lanes = x.shape[5]
    inner = x.shape[0] * x.shape[4]
    halves = [pl.ds(u * half, half) for u in range(2)]
    t0, d0 = place_ref[0], place_ref[1]
    spots = [(d, a) for d in range(2) for a in range(2)]
    one_loads = copies(one_sem, *[(one_hbm.at[:, rows], one.at[:, rows]) for rows in halves])
    two_loads = copies(two_sem, *[(two_hbm.at[:, rows], two.at[:, rows]) for rows in halves])
    held_loads = copies(held_sem, *[(held_hbm[n], held.at[:, :, pl.ds(n * half, half)]) for n in range(2)])
    one_loads[0].start()
    for load in one_loads[1:] + two_loads + held_loads:
        load.start()

    for t in range(2):
        one_loads[t].wait()
        for d, a in spots:
            vr = x[:, 0, a, d].reshape(inner, lanes)
            vi = x[:, 1, a, d].reshape(inner, lanes)
            yr, yi = complex_dot(one[0, halves[t], :], one[1, halves[t], :], vr, vi)
            first[d, a, t, 0] = yr.astype(BF)
            first[d, a, t, 1] = yi.astype(BF)

    for u in range(2):
        two_loads[u].wait()

        def step_two(n, _):
            for t, out in ((t0, v), (1 - t0, v_out)):
                vr = first[n, :, t, 0].reshape(2 * half, lanes)
                vi = first[n, :, t, 1].reshape(2 * half, lanes)
                yr, yi = complex_dot(two[0, halves[u], :], two[1, halves[u], :], vr, vi)
                out[n, 0, u] = yr.astype(BF)
                out[n, 1, u] = yi.astype(BF)
            return 0

        lax.fori_loop(0, 2, step_two, 0)

    for load in held_loads:
        load.wait()
    for u in range(2):
        vr = jnp.concatenate([v[d0, 0, u], v[1 - d0, 0, u]], axis=0)
        vi = jnp.concatenate([v[d0, 1, u], v[1 - d0, 1, u]], axis=0)
        part[u, 0], part[u, 1] = complex_dot(held[0], held[1], vr, vi)


def chained(place, x, one, two, held):
    half = one.shape[1] // 2
    lanes = x.shape[5]
    rows = held[0].shape[1]
    v_shape = (2, 2, 2, half, lanes)
    part_shape = (2, 2, rows, lanes)
    sems = lambda count: pltpu.SemaphoreType.DMA((count,))
    return pl.pallas_call(
        chain_kernel,
        in_specs=[pl.BlockSpec(memory_space=pltpu.SMEM)] + inside(1) + anywhere(4),
        out_specs=inside(2),
        out_shape=[pltpu.VMEM(v_shape, BF), pltpu.VMEM(part_shape, F32)],
        scratch_shapes=[
            pltpu.VMEM(one.shape, BF),
            pltpu.VMEM(two.shape, BF),
            pltpu.VMEM((2, rows, 2 * half), BF),
            pltpu.VMEM((2,) + v_shape, BF),
            pltpu.VMEM(v_shape, BF),
        ] + [sems(2), sems(2), sems(2)],
        cost_estimate=pl.CostEstimate(flops=112 * half * half * 2 * lanes, transcendentals=0, bytes_accessed=72 * half**2),
        compiler_params=params(28),
        name="chain",
    )(place, x, one, two, *held)


def join_kernel(place_ref, w_own, w_other, v, part, out):
    lanes = v.shape[4]
    d0 = place_ref[1]
    wr, wi = (jnp.concatenate([w_own[r], w_other[r]], axis=1) for r in range(2))
    for u in range(2):
        vr = jnp.concatenate([v[d0, 0, u], v[1 - d0, 0, u]], axis=0)
        vi = jnp.concatenate([v[d0, 1, u], v[1 - d0, 1, u]], axis=0)
        yr, yi = complex_dot(wr, wi, vr, vi)
        for r, y in enumerate((yr, yi)):
            out[:, (2 * r + u) * lanes:(2 * r + u + 1) * lanes] = (part[u, r] + y).astype(BF)


def joined(place, weights, v, part):
    rows, inner = weights[0].shape[1:]
    lanes = v.shape[4]
    return pl.pallas_call(
        join_kernel,
        in_specs=[pl.BlockSpec(memory_space=pltpu.SMEM)] + inside(4),
        out_specs=inside(1)[0],
        out_shape=jax.ShapeDtypeStruct((rows, 4 * lanes), BF),
        cost_estimate=pl.CostEstimate(flops=32 * rows * inner * lanes, transcendentals=0, bytes_accessed=24 * rows * inner),
        compiler_params=params(16),
        name="join",
    )(place, *weights, v, part)


def pick_kernel(own_ref, pick_ref, branch_hbm, out_hbm, held, sem, out_sem):
    spot = pick_ref[own_ref[0]]
    loads = copies(sem, *[(branch_hbm.at[spot, r, 0], held.at[r]) for r in range(2)])
    stores = copies(out_sem, *[(held.at[r], out_hbm.at[r]) for r in range(2)])
    for load in loads:
        load.start()
    for load, store in zip(loads, stores):
        load.wait()
        store.start()
    for store in stores:
        store.wait()


def picked(own, slice_pick, branch):
    smem = pl.BlockSpec(memory_space=pltpu.SMEM)
    return pl.pallas_call(
        pick_kernel,
        in_specs=[smem, smem] + anywhere(1),
        out_specs=anywhere(1)[0],
        out_shape=jax.ShapeDtypeStruct(branch.shape[1:2] + branch.shape[3:], BF),
        scratch_shapes=[
            pltpu.VMEM(branch.shape[1:2] + branch.shape[3:], BF),
            pltpu.SemaphoreType.DMA((2,)),
            pltpu.SemaphoreType.DMA((2,)),
        ],
        cost_estimate=pl.CostEstimate(flops=0, transcendentals=0, bytes_accessed=2 * branch.size),
        compiler_params=params(4),
        name="pick",
    )(own.reshape(1).astype(jnp.int32), slice_pick, branch)


def per_device(stem, branch_one, branch_two, branch_three, leg_orders, slice_pick):
    groups = lax.axis_size("modes")
    own = lax.axis_index("modes")
    side = groups // 2
    quarter = groups // 4
    extent = stem.shape[2]
    lanes = stem.shape[4]
    leg_width = branch_one.shape[2]
    top = own // side
    core = own % 2
    middle = (own // quarter == 1) | (own // quarter == 2)

    beside = [(i, i ^ 1) for i in range(groups)]
    swap = [(a * quarter + i, b * quarter + i) for a, b in ((1, 2), (2, 1)) for i in range(quarter)]
    cycle = [(a * quarter + i, b * quarter + i) for a, b in ((0, 2), (2, 3), (3, 1), (1, 0)) for i in range(quarter)]

    chosen = picked(own, slice_pick, branch_three)
    out_width = chosen.shape[1]
    share = out_width // groups
    chosen, stem = lax.optimization_barrier((chosen, stem))

    def move(value, route):
        return lax.ppermute(value, "modes", route)

    swapped = move(chosen, swap)
    near = move(chosen, beside)

    pieces = stem.reshape(2, extent, 2, side, 2, lanes).transpose(3, 0, 2, 4, 1, 5)
    halves = [list(range(side)), list(range(side, groups))]
    arrived = lax.all_to_all(pieces, "modes", 0, 0, tiled=True, axis_index_groups=halves)
    if extent % 16:
        arrived = arrived.transpose(1, 2, 3, 0, 4, 5).reshape(1, 2, 2, 2, side * extent, lanes)

    start = (top * (leg_width // 2)).reshape(1).astype(jnp.int32)
    place = jnp.stack([top, core]).astype(jnp.int32)
    one = turned(0, start, leg_width // 2, leg_orders, branch_one)
    two = turned(1, jnp.zeros_like(start), leg_width, leg_orders, branch_two)
    swapped, one, two = lax.optimization_barrier((swapped, one, two))
    other = move(jnp.where(middle, swapped, chosen), cycle)
    v, part = chained(place, arrived, one, two, (chosen, near))
    other, v = lax.optimization_barrier((other, v))
    far = move(other, beside)
    partial = joined(place, (other, far), v, part)
    spread = lax.all_to_all(partial.reshape(groups, share, 4 * lanes), "modes", 0, 0, tiled=True)
    total = jnp.sum(spread.reshape(side, 2, share, 4 * lanes).astype(F32), axis=0).astype(BF)
    return total.reshape(2, share, 2, 2, lanes).transpose(1, 2, 3, 0, 4)


def solution(mesh):
    in_specs = (
        P(None, "modes", None, None, "parts"),
        P(),
        P(),
        P(None, None, "modes", None, None),
        P(),
        P("parts"),
    )
    out_specs = P(("parts", "modes"), None, None, None, None)

    return jax.shard_map(per_device, mesh=mesh, in_specs=in_specs, out_specs=out_specs, check_vma=False)
```

```python
import jax
import jax.numpy as jnp
from jax import lax
from jax.experimental import pallas as pl
from jax.experimental.pallas import tpu as pltpu
from jax.sharding import PartitionSpec as P


BF = jnp.bfloat16
F32 = jnp.float32


def dot(lhs, rhs):
    return jnp.dot(lhs, rhs, preferred_element_type=F32)


def copies(sem, *pairs):
    return [pltpu.make_async_copy(src, dst, sem.at[n]) for n, (src, dst) in enumerate(pairs)]


def params(mib):
    return pltpu.CompilerParams(vmem_limit_bytes=mib << 20)


def inside(count):
    return [pl.BlockSpec(memory_space=pltpu.VMEM) for _ in range(count)]


def anywhere(count):
    return [pl.BlockSpec(memory_space=pltpu.HBM) for _ in range(count)]


def complex_dot(wr, wi, vr, vi):
    return dot(wr, vr) - dot(wi, vi), dot(wr, vi) + dot(wi, vr)


def turn_kernel(row, start_ref, orders_ref, branch_hbm, out_hbm, branch, out, pick, sem, out_sem):
    leg_width, width = pick.shape
    half = leg_width // 2
    pieces = [(r, pl.ds(u * half, half)) for r in range(2) for u in range(2)]
    loads = copies(sem, *[(branch_hbm.at[r, rows], branch.at[r, rows]) for r, rows in pieces])
    stores = copies(out_sem, *[(out.at[r, rows], out_hbm.at[r, rows]) for r, rows in pieces])
    for load in loads:
        load.start()

    index = lax.broadcasted_iota(jnp.int32, (1, width), 1) + start_ref[0]
    placed = jnp.zeros((1, width), jnp.int32)
    for bit in range(leg_width.bit_length() - 1):
        placed += jnp.left_shift(jnp.right_shift(index, bit) & 1, orders_ref[row, bit])
    ahead = placed - lax.broadcasted_iota(jnp.int32, (16, width), 0)

    def build(n, _):
        base = pl.multiple_of(n * 16, 16)
        pick[pl.ds(base, 16), :] = jnp.where(ahead == base, 1.0, 0.0).astype(BF)
        return 0

    lax.fori_loop(0, leg_width // 16, build, 0)
    for (r, rows), load, store in zip(pieces, loads, stores):
        load.wait()
        out[r, rows, :] = dot(branch[r, rows, :], pick[...]).astype(BF)
        store.start()
    for store in stores:
        store.wait()


def turned(row, start, width, orders, branch):
    leg_width = branch.shape[2]
    smem = pl.BlockSpec(memory_space=pltpu.SMEM)
    return pl.pallas_call(
        lambda *refs: turn_kernel(row, *refs),
        in_specs=[smem, smem] + anywhere(1),
        out_specs=anywhere(1)[0],
        out_shape=jax.ShapeDtypeStruct((2, leg_width, width), BF),
        scratch_shapes=[
            pltpu.VMEM(branch.shape, BF),
            pltpu.VMEM((2, leg_width, width), BF),
            pltpu.VMEM((leg_width, width), BF),
            pltpu.SemaphoreType.DMA((4,)),
            pltpu.SemaphoreType.DMA((4,)),
        ],
        cost_estimate=pl.CostEstimate(flops=4 * width * leg_width**2, transcendentals=0, bytes_accessed=4 * leg_width**2),
        compiler_params=params(16),
        name="turn",
    )(start, orders, branch)


def chain_kernel(place_ref, x, one_hbm, two_hbm, *refs):
    held_hbm, (v_out, part) = refs[:2], refs[2:4]
    one, two, held, first, v, one_sem, two_sem, held_sem = refs[4:]
    half = one.shape[1] // 2
    lanes = x.shape[5]
    inner = x.shape[0] * x.shape[4]
    halves = [pl.ds(u * half, half) for u in range(2)]
    t0, d0 = place_ref[0], place_ref[1]
    spots = [(d, a) for d in range(2) for a in range(2)]
    one_loads = copies(one_sem, *[(one_hbm.at[:, rows], one.at[:, rows]) for rows in halves])
    two_loads = copies(two_sem, *[(two_hbm.at[:, rows], two.at[:, rows]) for rows in halves])
    held_loads = copies(held_sem, *[(held_hbm[n], held.at[:, :, pl.ds(n * half, half)]) for n in range(2)])
    one_loads[0].start()
    for load in one_loads[1:] + two_loads + held_loads:
        load.start()

    for t in range(2):
        one_loads[t].wait()
        for d, a in spots:
            vr = x[:, 0, a, d].reshape(inner, lanes)
            vi = x[:, 1, a, d].reshape(inner, lanes)
            yr, yi = complex_dot(one[0, halves[t], :], one[1, halves[t], :], vr, vi)
            first[d, a, t, 0] = yr.astype(BF)
            first[d, a, t, 1] = yi.astype(BF)

    for u in range(2):
        two_loads[u].wait()

        def step_two(n, _):
            for t, out in ((t0, v), (1 - t0, v_out)):
                vr = first[n, :, t, 0].reshape(2 * half, lanes)
                vi = first[n, :, t, 1].reshape(2 * half, lanes)
                yr, yi = complex_dot(two[0, halves[u], :], two[1, halves[u], :], vr, vi)
                out[n, 0, u] = yr.astype(BF)
                out[n, 1, u] = yi.astype(BF)
            return 0

        lax.fori_loop(0, 2, step_two, 0)

    for load in held_loads:
        load.wait()
    for u in range(2):
        vr = jnp.concatenate([v[d0, 0, u], v[1 - d0, 0, u]], axis=0)
        vi = jnp.concatenate([v[d0, 1, u], v[1 - d0, 1, u]], axis=0)
        part[u, 0], part[u, 1] = complex_dot(held[0], held[1], vr, vi)


def chained(place, x, one, two, held):
    half = one.shape[1] // 2
    lanes = x.shape[5]
    rows = held[0].shape[1]
    v_shape = (2, 2, 2, half, lanes)
    part_shape = (2, 2, rows, lanes)
    sems = lambda count: pltpu.SemaphoreType.DMA((count,))
    return pl.pallas_call(
        chain_kernel,
        in_specs=[pl.BlockSpec(memory_space=pltpu.SMEM)] + inside(1) + anywhere(4),
        out_specs=inside(2),
        out_shape=[pltpu.VMEM(v_shape, BF), pltpu.VMEM(part_shape, F32)],
        scratch_shapes=[
            pltpu.VMEM(one.shape, BF),
            pltpu.VMEM(two.shape, BF),
            pltpu.VMEM((2, rows, 2 * half), BF),
            pltpu.VMEM((2,) + v_shape, BF),
            pltpu.VMEM(v_shape, BF),
        ] + [sems(2), sems(2), sems(2)],
        cost_estimate=pl.CostEstimate(flops=112 * half * half * 2 * lanes, transcendentals=0, bytes_accessed=72 * half**2),
        compiler_params=params(28),
        name="chain",
    )(place, x, *[pltpu.with_memory_space_constraint(value, pltpu.HBM) for value in (one, two, *held)])


def join_kernel(place_ref, w_own, w_other, v, part, *refs):
    outs, rest = refs[:-1], refs[-1]
    halves, chips, cores, share = rest.shape[:4]
    lanes = v.shape[4]
    count = chips * cores * share
    top, core, chip = place_ref[0], place_ref[1], place_ref[2]
    for h in range(halves):
        rows = pl.ds(h * count, count)
        wr, wi = (jnp.concatenate([w_own[r, rows, :], w_other[r, rows, :]], axis=1) for r in range(2))
        for u in range(2):
            vr = jnp.concatenate([v[core, 0, u], v[1 - core, 0, u]], axis=0)
            vi = jnp.concatenate([v[core, 1, u], v[1 - core, 1, u]], axis=0)
            yr, yi = complex_dot(wr, wi, vr, vi)
            for r, y in enumerate((yr, yi)):
                total = (part[u, r, rows, :] + y).astype(BF)
                columns = pl.ds((2 * r + u) * lanes, lanes)
                for n in range(chips * cores):
                    rest[h, n // cores, n % cores, :, columns] = total[n * share:(n + 1) * share]
    for n, out in enumerate(outs):
        for e in range(cores):
            out[e] = rest[1 - top if n < chips else top, chip ^ (n % chips), core ^ e]


def joined(groups, place, weights, v, part):
    rows, inner = weights[0].shape[1:]
    lanes = v.shape[4]
    outs = pl.pallas_call(
        join_kernel,
        in_specs=[pl.BlockSpec(memory_space=pltpu.SMEM)] + inside(4),
        out_specs=inside(groups // 2),
        out_shape=[jax.ShapeDtypeStruct((2, rows // groups, 4 * lanes), BF)] * (groups // 2),
        scratch_shapes=[pltpu.VMEM((2, groups // 4, 2, rows // groups, 4 * lanes), BF)],
        cost_estimate=pl.CostEstimate(flops=32 * rows * inner * lanes, transcendentals=0, bytes_accessed=24 * rows * inner),
        compiler_params=params(16),
        name="join",
    )(place, *weights, v, part)
    return outs[:groups // 4], outs[groups // 4:]


def pick_kernel(own_ref, pick_ref, branch_hbm, out_hbm, held, sem, out_sem):
    spot = pick_ref[own_ref[0]]
    loads = copies(sem, *[(branch_hbm.at[spot, r, 0], held.at[r]) for r in range(2)])
    stores = copies(out_sem, *[(held.at[r], out_hbm.at[r]) for r in range(2)])
    for load in loads:
        load.start()
    for load, store in zip(loads, stores):
        load.wait()
        store.start()
    for store in stores:
        store.wait()


def picked(own, slice_pick, branch):
    smem = pl.BlockSpec(memory_space=pltpu.SMEM)
    return pl.pallas_call(
        pick_kernel,
        in_specs=[smem, smem] + anywhere(1),
        out_specs=anywhere(1)[0],
        out_shape=jax.ShapeDtypeStruct(branch.shape[1:2] + branch.shape[3:], BF),
        scratch_shapes=[
            pltpu.VMEM(branch.shape[1:2] + branch.shape[3:], BF),
            pltpu.SemaphoreType.DMA((2,)),
            pltpu.SemaphoreType.DMA((2,)),
        ],
        cost_estimate=pl.CostEstimate(flops=0, transcendentals=0, bytes_accessed=2 * branch.size),
        compiler_params=params(4),
        name="pick",
    )(own.reshape(1).astype(jnp.int32), slice_pick, branch)


def relay_kernel(middle_ref, swapped, chosen, out):
    @pl.when(middle_ref[0] == 1)
    def _():
        out[...] = swapped[...]

    @pl.when(middle_ref[0] == 0)
    def _():
        out[...] = chosen[...]


def relayed(middle, swapped, chosen):
    return pl.pallas_call(
        relay_kernel,
        in_specs=[pl.BlockSpec(memory_space=pltpu.SMEM)] + inside(2),
        out_specs=inside(1)[0],
        out_shape=jax.ShapeDtypeStruct(chosen.shape, BF),
        cost_estimate=pl.CostEstimate(flops=0, transcendentals=0, bytes_accessed=6 * chosen.size),
        compiler_params=params(8),
        name="relay",
    )(middle.reshape(1).astype(jnp.int32), swapped, chosen)


def per_device(stem, branch_one, branch_two, branch_three, leg_orders, slice_pick):
    groups = lax.axis_size("modes")
    own = lax.axis_index("modes")
    side = groups // 2
    quarter = groups // 4
    extent = stem.shape[2]
    lanes = stem.shape[4]
    leg_width = branch_one.shape[2]
    top = own // side
    core = own % 2
    middle = (own // quarter == 1) | (own // quarter == 2)

    beside = [(i, i ^ 1) for i in range(groups)]
    swap = [(a * quarter + i, b * quarter + i) for a, b in ((1, 2), (2, 1)) for i in range(quarter)]
    cycle = [(a * quarter + i, b * quarter + i) for a, b in ((0, 2), (2, 3), (3, 1), (1, 0)) for i in range(quarter)]

    chosen = picked(own, slice_pick, branch_three)
    out_width = chosen.shape[1]
    share = out_width // groups
    chosen, stem = lax.optimization_barrier((chosen, stem))

    def move(value, route):
        return lax.ppermute(value, "modes", route)

    swapped = move(chosen, swap)
    near = move(chosen, beside)

    pieces = stem.reshape(2, extent, 2, side, 2, lanes).transpose(3, 0, 2, 4, 1, 5)
    halves = [list(range(side)), list(range(side, groups))]
    arrived = lax.all_to_all(pieces, "modes", 0, 0, tiled=True, axis_index_groups=halves)
    if extent % 16:
        arrived = arrived.transpose(1, 2, 3, 0, 4, 5).reshape(1, 2, 2, 2, side * extent, lanes)

    start = (top * (leg_width // 2)).reshape(1).astype(jnp.int32)
    place = jnp.stack([top, core, own % side // 2]).astype(jnp.int32)
    one = turned(0, start, leg_width // 2, leg_orders, branch_one)
    two = turned(1, jnp.zeros_like(start), leg_width, leg_orders, branch_two)
    swapped, one, two = lax.optimization_barrier((swapped, one, two))
    other = move(relayed(middle, swapped, chosen), cycle)
    v, part = chained(place, arrived, one, two, (chosen, near))
    other, v = lax.optimization_barrier((other, v))
    far = move(other, beside)
    weights = (other, far)

    def relative(offset):
        return [(i, i ^ offset) for i in range(groups)]

    def exchanged(sent):
        return [move(sent[s], relative(2 * s)) for s in range(1, groups // 4)]

    def added(sent, came):
        total = sent[0].astype(F32)
        for piece in came:
            total = total + piece.astype(F32)
        return total

    push, pull = joined(groups, place, weights, v, part)
    pushed = exchanged(push)
    pulled = exchanged(pull)
    crossing = added(push, pushed).astype(BF)
    straight = move(crossing[0], relative(side))
    slanted = move(crossing[1], relative(side + 1))
    kept = added(pull, pulled)
    passed = move(kept[1].astype(BF), beside)
    mine = (kept[0] + straight.astype(F32)).astype(BF).reshape(share, 2, 2, lanes)
    yours = (passed.astype(F32) + slanted.astype(F32)).astype(BF).reshape(share, 2, 2, lanes)
    return jnp.where(core == 0, jnp.stack([mine, yours], axis=3), jnp.stack([yours, mine], axis=3))


def solution(mesh):
    in_specs = (
        P(None, "modes", None, None, "parts"),
        P(),
        P(),
        P(None, None, "modes", None, None),
        P(),
        P("parts"),
    )
    out_specs = P(("parts", "modes"), None, None, None, None)

    return jax.shard_map(per_device, mesh=mesh, in_specs=in_specs, out_specs=out_specs, check_vma=False)
```
